256 devices in a mesh: section: 32 (over y, z_lo, core), tensor: 8 (over z_hi, x).
Axes of the slice: x: 4, y: 4, z: 8 (z_hi: 2, z_lo: 4; z = z_hi * 4 + z_lo), core: 2. Of those that a mesh axis runs over, the one named last changes fastest.
Arguments:
- saved: bfloat16 [32, 32, 64, 8192], P('section', None, 'tensor'), may hold values from -6 to 6
- offsets: int32 [32, 32], P('section'), may hold values from 0 to 31, as said below
Outputs:
- restored: float32 [32, 32, 64, 8192], P('section', None, None, 'tensor')
- block_sums: float32 [32, 32, 8192], P('section', None, 'tensor')
The draws below stay inside these ranges and needn't reach their ends.
Inputs may be any that keep to these rules, and one draw needn't show every extreme that they name: Each row of offsets is a permutation of 0 to 31.
All inputs are finite; a program needn't handle non-finite values.
Results may differ from the reference program's by a relative error of at most 0.0003.
Values may be sent and summed in bfloat16 or wider, within the bound.
A program may use at most 128 MiB of HBM per device.

```python
import jax
import jax.numpy as jnp

D = 8192
R = 64
SLOTS = 32
N_SECTION = 32


def draw_offsets(key, part):
    row_keys = jax.random.split(jax.random.fold_in(key, 17), N_SECTION)
    rows = jax.vmap(lambda k: jax.random.permutation(k, N_SECTION))(row_keys)
    return rows.astype(jnp.int32)


def shard_levels(stream_key, dims, cuts, least, largest):
    def one(dim, parts):
        draws = jax.random.uniform(jax.random.fold_in(jax.random.fold_in(stream_key, 6), dim), (parts,), jnp.float32, least / len(cuts), largest / len(cuts))
        return jnp.repeat(jnp.exp(draws), dims[dim] // parts).reshape((-1,) + (1,) * (len(dims) - dim - 1))

    factor_of = one(*cuts[0])
    for cut in cuts[1:]:
        factor_of = factor_of * one(*cut)
    return factor_of


def gaussian(stream_key, dims, width, limit, cuts=(), kind=jnp.bfloat16):
    loudness = shard_levels(stream_key, dims, cuts, -0.22, 0.18) if cuts else 1.0
    entries = jax.random.normal(stream_key, dims, jnp.float32) * width * loudness
    return jnp.minimum(jnp.maximum(entries, -limit), limit).astype(kind)


def setup_inputs(seed: int = 0) -> dict:
    keys = jax.random.split(jax.random.key(seed), 3)
    return {
        "saved": gaussian(keys[0], (N_SECTION, SLOTS, R, D), 1.0, 6.0, ((0, 32), (2, 8))),
        "offsets": draw_offsets(jax.random.fold_in(keys[2], 71), 0),
    }


def reference(saved, offsets):
    sections = jnp.arange(N_SECTION, dtype=jnp.int32)
    relative = ((sections[:, None] - sections[None, :]) % N_SECTION).astype(jnp.int32)
    inverse = jnp.argsort(offsets, axis=1).astype(jnp.int32)
    sources = jnp.broadcast_to(sections[None, :], (N_SECTION, N_SECTION)).astype(jnp.int32)
    chosen = inverse[sources, relative]
    blocks = saved[sources, chosen]
    restored = blocks.astype(jnp.float32)
    block_sums = jnp.sum(restored, axis=2)
    return restored, block_sums
```

```python
import jax
import jax.numpy as jnp
from jax import lax
from jax.experimental import pallas as pl
from jax.experimental.pallas import tpu as pltpu
from jax.sharding import PartitionSpec as P

MESH = pl.DeviceIdType.MESH
MIB = 1 << 20
FAR_FIRST = (2, 1, 3)
Z_ORDER = (4, 3, 5, 2, 6, 1, 7)


def exchange(saved, offsets, dst, raw, src, table, slot, load_sem, table_sem, send_sem, recv_sem, second, third):
    section, tensor = lax.axis_index("section"), lax.axis_index("tensor")
    y, z_lo, core = lax.div(section, 8), lax.rem(lax.div(section, 2), 4), lax.rem(section, 2)
    z_hi, x = lax.div(tensor, 4), lax.rem(tensor, 4)
    z = z_hi * 4 + z_lo

    def device(dx, dy, dz, dc):
        tx, ty, tz, tc = lax.rem(x + dx, 4), lax.rem(y + dy, 4), lax.rem(z + dz, 8), lax.rem(core + dc, 2)
        return (ty * 4 + lax.rem(tz, 4)) * 2 + tc, lax.div(tz, 4) * 4 + tx

    def signal(semaphore, *offset):
        pl.semaphore_signal(semaphore, inc=1, device_id=device(*offset), device_id_type=MESH)

    def send(*offset):
        to = device(*offset)
        columns = pl.ds(pl.multiple_of(to[1] * 1024, 1024), 1024)
        pltpu.make_async_remote_copy(
            src_ref=src.at[to[0], :, columns],
            dst_ref=dst.at[section * 8 + tensor],
            send_sem=send_sem,
            recv_sem=recv_sem,
            device_id=to,
            device_id_type=MESH,
        ).start()

    def loop(count, step):
        lax.fori_loop(0, count, lambda i, carry: (step(i), carry)[1], 0)

    barrier = pltpu.get_barrier_semaphore()
    for dz in Z_ORDER:
        signal(barrier, 0, 0, dz, 0)
    for d in FAR_FIRST:
        signal(barrier, 0, d, 0, 0)
        signal(barrier, d, 0, 0, 0)
    signal(barrier, 0, 0, 0, 1)

    read = pltpu.make_async_copy(offsets, table, table_sem)
    read.start()
    load = pltpu.make_async_copy(saved, raw, load_sem)
    load.start()
    read.wait()

    def find(t):
        wanted = lax.rem(t - section + 32, 32)
        found = jnp.int32(0)
        for j in range(32):
            found = jnp.where(table[0, j] == wanted, jnp.int32(j), found)
        slot[t] = found

    loop(32, find)
    load.wait()

    def place(t):
        src[t] = raw[slot[t]]

    loop(32, place)
    dst[section * 8 + tensor] = src[section, :, pl.ds(pl.multiple_of(tensor * 1024, 1024), 1024)]
    pl.semaphore_wait(barrier, 14)

    for d in FAR_FIRST:
        signal(second, 0, d, 0, 0)
        signal(second, d, 0, 0, 0)
    for dz in Z_ORDER:
        send(0, 0, dz, 0)
    for d in FAR_FIRST:
        send(0, d, 0, 0)
        send(d, 0, 0, 0)
    send(0, 0, 0, 1)
    pl.semaphore_wait(second, 6)

    for d in FAR_FIRST:
        signal(third, d, 0, 0, 1)
    signal(third, 0, 0, 0, 1)
    for d in FAR_FIRST:
        signal(third, d, 0, 0, 0)

    def far(i):
        return 2 - i + 3 * lax.div(i, 2)

    def two_lines(i):
        along_y = lax.div(i, 3)
        d = far(lax.rem(i, 3))
        dx, dy = d * (1 - along_y), d * along_y
        for dz in Z_ORDER:
            send(dx, dy, dz, 0)
        send(dx, dy, 0, 1)

    loop(6, two_lines)
    loop(9, lambda i: send(far(lax.rem(i, 3)), far(lax.div(i, 3)), 0, 0))
    pl.semaphore_wait(third, 7)

    def corner(i):
        dx, dy = far(lax.rem(i, 3)), far(lax.div(i, 3))
        for dc in (1, 0):
            for dz in Z_ORDER:
                send(dx, dy, dz, dc)
        send(dx, dy, 0, 1)

    loop(9, corner)

    def other_core(i):
        along_y = lax.div(i, 3)
        d = far(lax.rem(i, 3))
        dx, dy = d * (1 - along_y), d * along_y
        for dz in Z_ORDER:
            send(dx, dy, dz, 1)

    loop(6, other_core)
    for dz in Z_ORDER:
        send(0, 0, dz, 1)

    others = dst.at[pl.ds(0, 255)]
    pltpu.make_async_copy(others, others, recv_sem).wait()
    pltpu.make_async_copy(others, others, send_sem).wait()


def widen(arrived, restored, sums, wide, store_sem):
    def step(s, carry):
        block = arrived[pl.ds(pl.multiple_of(s * 8, 8), 8)].astype(jnp.float32).reshape(64, 1024)
        wide[s] = block
        pltpu.make_async_copy(wide.at[s], restored.at[s], store_sem).start()
        sums[s] = jnp.sum(block, axis=0)
        return carry

    lax.fori_loop(0, 32, step, 0)
    pltpu.make_async_copy(wide, restored, store_sem).wait()


def body(saved, offsets):
    arrived = pl.pallas_call(
        exchange,
        out_shape=pltpu.VMEM((256, 8, 1024), jnp.bfloat16),
        in_specs=[pl.BlockSpec(memory_space=pltpu.HBM), pl.BlockSpec(memory_space=pltpu.HBM)],
        out_specs=pl.BlockSpec(memory_space=pltpu.VMEM),
        scratch_shapes=[
            pltpu.VMEM((32, 8, 8192), jnp.bfloat16),
            pltpu.VMEM((32, 8, 8192), jnp.bfloat16),
            pltpu.SMEM((1, 32), jnp.int32),
            pltpu.SMEM((32,), jnp.int32),
            pltpu.SemaphoreType.DMA,
            pltpu.SemaphoreType.DMA,
            pltpu.SemaphoreType.DMA,
            pltpu.SemaphoreType.DMA,
            pltpu.SemaphoreType.REGULAR,
            pltpu.SemaphoreType.REGULAR,
        ],
        compiler_params=pltpu.CompilerParams(collective_id=0, has_side_effects=True, vmem_limit_bytes=62849024),
    )(saved[0], offsets)
    restored, block_sums = pl.pallas_call(
        widen,
        out_shape=(
            jax.ShapeDtypeStruct((32, 64, 1024), jnp.float32),
            jax.ShapeDtypeStruct((32, 1024), jnp.float32),
        ),
        in_specs=[pl.BlockSpec(memory_space=pltpu.VMEM)],
        out_specs=(pl.BlockSpec(memory_space=pltpu.HBM), pl.BlockSpec(memory_space=pltpu.VMEM)),
        scratch_shapes=[pltpu.VMEM((32, 64, 1024), jnp.float32), pltpu.SemaphoreType.DMA],
        compiler_params=pltpu.CompilerParams(vmem_limit_bytes=24 * MIB),
    )(arrived)
    return (restored[None], block_sums[None])


def solution(mesh):
    return jax.shard_map(
        body,
        mesh=mesh,
        in_specs=(P("section", None, "tensor", None), P("section", None)),
        out_specs=(P("section", None, None, "tensor"), P("section", None, "tensor")),
        check_vma=False,
    )
```

```python
import jax
import jax.numpy as jnp
from jax import lax
from jax.experimental import pallas as pl
from jax.experimental.pallas import tpu as pltpu
from jax.sharding import PartitionSpec as P

MESH = pl.DeviceIdType.MESH
MIB = 1 << 20
FAR_FIRST = (2, 1, 3)
Z_ORDER = (4, 3, 5, 2, 6, 1, 7)


def exchange(saved, offsets, dst, raw, src, table, slot, load_sem, table_sem, send_sem, recv_sem, second, third):
    section, tensor = lax.axis_index("section"), lax.axis_index("tensor")
    y, z_lo, core = lax.div(section, 8), lax.rem(lax.div(section, 2), 4), lax.rem(section, 2)
    z_hi, x = lax.div(tensor, 4), lax.rem(tensor, 4)
    z = z_hi * 4 + z_lo

    def device(dx, dy, dz, dc):
        tx, ty, tz, tc = lax.rem(x + dx, 4), lax.rem(y + dy, 4), lax.rem(z + dz, 8), lax.rem(core + dc, 2)
        return (ty * 4 + lax.rem(tz, 4)) * 2 + tc, lax.div(tz, 4) * 4 + tx

    def signal(semaphore, *offset):
        pl.semaphore_signal(semaphore, inc=1, device_id=device(*offset), device_id_type=MESH)

    def send(*offset):
        to = device(*offset)
        columns = pl.ds(pl.multiple_of(to[1] * 1024, 1024), 1024)
        pltpu.make_async_remote_copy(
            src_ref=src.at[to[0], :, columns],
            dst_ref=dst.at[section * 8 + tensor],
            send_sem=send_sem,
            recv_sem=recv_sem,
            device_id=to,
            device_id_type=MESH,
        ).start()

    def loop(count, step):
        lax.fori_loop(0, count, lambda i, carry: (step(i), carry)[1], 0)

    barrier = pltpu.get_barrier_semaphore()
    read = pltpu.make_async_copy(offsets, table, table_sem)
    read.start()
    load = pltpu.make_async_copy(saved, raw, load_sem)
    load.start()
    for dz in Z_ORDER:
        signal(barrier, 0, 0, dz, 0)
    for d in FAR_FIRST:
        signal(barrier, 0, d, 0, 0)
        signal(barrier, d, 0, 0, 0)
    signal(barrier, 0, 0, 0, 1)

    read.wait()

    def find(t):
        wanted = lax.rem(t - section + 32, 32)
        found = jnp.int32(0)
        for j in range(32):
            found = jnp.where(table[0, j] == wanted, jnp.int32(j), found)
        slot[t] = found

    loop(32, find)
    load.wait()

    def place(t):
        src[t] = raw[slot[t]]

    loop(32, place)
    dst[section * 8 + tensor] = src[section, :, pl.ds(pl.multiple_of(tensor * 1024, 1024), 1024)]
    pl.semaphore_wait(barrier, 14)

    for d in FAR_FIRST:
        signal(second, 0, d, 0, 0)
        signal(second, d, 0, 0, 0)
    for dz in Z_ORDER:
        send(0, 0, dz, 0)
    for d in FAR_FIRST:
        send(0, d, 0, 0)
        send(d, 0, 0, 0)
    send(0, 0, 0, 1)
    pl.semaphore_wait(second, 6)

    for d in FAR_FIRST:
        signal(third, d, 0, 0, 1)
    signal(third, 0, 0, 0, 1)
    for d in FAR_FIRST:
        signal(third, d, 0, 0, 0)

    def far(i):
        return 2 - i + 3 * lax.div(i, 2)

    def two_lines(i):
        along_y = lax.div(i, 3)
        d = far(lax.rem(i, 3))
        dx, dy = d * (1 - along_y), d * along_y
        for dz in Z_ORDER:
            send(dx, dy, dz, 0)
        send(dx, dy, 0, 1)

    loop(6, two_lines)
    loop(9, lambda i: send(far(lax.rem(i, 3)), far(lax.div(i, 3)), 0, 0))
    pl.semaphore_wait(third, 7)

    def corner(i):
        dx, dy = far(lax.rem(i, 3)), far(lax.div(i, 3))
        for dc in (1, 0):
            for dz in Z_ORDER:
                send(dx, dy, dz, dc)
        send(dx, dy, 0, 1)

    loop(9, corner)

    def other_core(i):
        along_y = lax.div(i, 3)
        d = far(lax.rem(i, 3))
        dx, dy = d * (1 - along_y), d * along_y
        for dz in Z_ORDER:
            send(dx, dy, dz, 1)

    loop(6, other_core)
    for dz in Z_ORDER:
        send(0, 0, dz, 1)

    others = dst.at[pl.ds(0, 255)]
    pltpu.make_async_copy(others, others, recv_sem).wait()
    pltpu.make_async_copy(others, others, send_sem).wait()


def widen(arrived, restored, sums, wide, total, store_sem, sum_sem):
    def step(s, carry):
        block = arrived[pl.ds(pl.multiple_of(s * 8, 8), 8)].astype(jnp.float32).reshape(64, 1024)
        wide[s] = block
        pltpu.make_async_copy(wide.at[s], restored.at[s], store_sem).start()
        total[s] = jnp.sum(block, axis=0)
        return carry

    lax.fori_loop(0, 32, step, 0)
    written = pltpu.make_async_copy(total, sums, sum_sem)
    written.start()
    pltpu.make_async_copy(wide, restored, store_sem).wait()
    written.wait()


def body(saved, offsets):
    arrived = pl.pallas_call(
        exchange,
        out_shape=pltpu.VMEM((256, 8, 1024), jnp.bfloat16),
        in_specs=[pl.BlockSpec(memory_space=pltpu.HBM), pl.BlockSpec(memory_space=pltpu.HBM)],
        out_specs=pl.BlockSpec(memory_space=pltpu.VMEM),
        scratch_shapes=[
            pltpu.VMEM((32, 8, 8192), jnp.bfloat16),
            pltpu.VMEM((32, 8, 8192), jnp.bfloat16),
            pltpu.SMEM((1, 32), jnp.int32),
            pltpu.SMEM((32,), jnp.int32),
            pltpu.SemaphoreType.DMA,
            pltpu.SemaphoreType.DMA,
            pltpu.SemaphoreType.DMA,
            pltpu.SemaphoreType.DMA,
            pltpu.SemaphoreType.REGULAR,
            pltpu.SemaphoreType.REGULAR,
        ],
        compiler_params=pltpu.CompilerParams(collective_id=0, has_side_effects=True, vmem_limit_bytes=62849024),
    )(saved[0], offsets)
    restored, block_sums = pl.pallas_call(
        widen,
        out_shape=(
            jax.ShapeDtypeStruct((32, 64, 1024), jnp.float32),
            jax.ShapeDtypeStruct((32, 1024), jnp.float32),
        ),
        in_specs=[pl.BlockSpec(memory_space=pltpu.VMEM)],
        out_specs=(pl.BlockSpec(memory_space=pltpu.HBM), pl.BlockSpec(memory_space=pltpu.HBM)),
        scratch_shapes=[
            pltpu.VMEM((32, 64, 1024), jnp.float32),
            pltpu.VMEM((32, 1024), jnp.float32),
            pltpu.SemaphoreType.DMA,
            pltpu.SemaphoreType.DMA,
        ],
        compiler_params=pltpu.CompilerParams(vmem_limit_bytes=24 * MIB),
    )(arrived)
    return (restored[None], block_sums[None])


def solution(mesh):
    return jax.shard_map(
        body,
        mesh=mesh,
        in_specs=(P("section", None, "tensor", None), P("section", None)),
        out_specs=(P("section", None, None, "tensor"), P("section", None, "tensor")),
        check_vma=False,
    )
```
